32 devices in a mesh: patch: 32 (over z, y, x, core).
Axes of the slice: x: 2, y: 2, z: 4, core: 2. Of those that a mesh axis runs over, the one named last changes fastest.
Arguments:
- positions: float32 [3, 65536], P(None, 'patch'), may hold values from -6 to 6
- densities: float32 [3, 65536], P(None, 'patch'), may hold values from -6 to 6
- near_src: int32 [512, 8], P('patch'), may hold values from 0 to 511, as said below
- near_count: int32 [512], P('patch'), may hold values from 1 to 8
- far_slot: int32 [512, 32], P('patch'), may hold values from 0 to 127
- far_class: int32 [512, 32], P('patch'), may hold values from 0 to 188
- far_count: int32 [512], P('patch'), may hold values from 1 to 32
- requests: int32 [32, 32, 4], P('patch'), may hold values from 0 to 15, as said below
- up_basis: bfloat16 [512, 144, 384], P('patch'), may hold values from -0.3125 to 0.3125
- transfer_table: bfloat16 [189, 20736], replicated, may hold values from -0.5 to 0.5
- down_basis: bfloat16 [512, 144, 9, 128], P('patch'), may hold values from -0.09375 to 0.09375
Outputs:
- shape_grad: float32 [3, 65536], P(None, 'patch')
The draws below stay inside these ranges and needn't reach their ends.
Inputs may be any that keep to these rules, and one draw needn't show every extreme that they name: `near_src`: the source leaf of each near-field block is held by the device of its target leaf or by the device just before or after it along patch. `requests`: each row names 4 different leaves of the source device, by their index on that device.
All inputs are finite; a program needn't handle non-finite values.
Results may differ from the reference program's by a relative error of at most 0.0042.
Values may be sent and summed in bfloat16 or wider, within the bound.
A program may use at most 192 MiB of HBM per device.

```python
import math
import jax
import jax.numpy as jnp
from jax import lax

P_SIZE = 128
RANK = 48
LEAF_DEV = 16
NEAR = 8
FAR = 32
CLASSES = 189
CAP = 4
LEAVES = 512
NODES = 65536
SLOTS = 128
N_PATCH = 32


def draw_near_src(key, part):
    leaves = jnp.arange(LEAVES, dtype=jnp.int32)
    owner = leaves // LEAF_DEV
    last_dev = LEAVES // LEAF_DEV - 1
    span = jnp.where((owner == 0) | (owner == last_dev), 2 * LEAF_DEV, 3 * LEAF_DEV)
    lowest = jnp.where(owner == 0, 0, (owner - 1) * LEAF_DEV)
    raw = jax.random.randint(jax.random.fold_in(key, 11), (LEAVES, NEAR), 0, 1 << 30)
    return (lowest[:, None] + raw % span[:, None]).astype(jnp.int32)


def draw_near_count(key, part):
    first, second, third = jax.random.split(jax.random.fold_in(key, 12), 3)
    ndev = LEAVES // LEAF_DEV
    level = jax.random.randint(first, (ndev,), max(1, NEAR // 4), NEAR + 1)
    raw = jax.random.randint(second, (LEAVES,), 0, 1 << 30)
    count = 1 + raw % jnp.repeat(level, LEAF_DEV)
    chosen = jax.random.randint(third, (), 0, ndev)
    leaves = jnp.arange(LEAVES, dtype=jnp.int32)
    return jnp.where(leaves == chosen * LEAF_DEV, NEAR, count).astype(jnp.int32)


def draw_requests(key, part):
    ndev = LEAVES // LEAF_DEV
    scores = jax.random.randint(jax.random.fold_in(key, 13), (ndev, ndev, LEAF_DEV), 0, 1 << 20)
    scores = scores * LEAF_DEV + jnp.arange(LEAF_DEV, dtype=jnp.int32)
    order = jnp.argsort(scores, axis=-1, stable=True)
    return order[:, :, :CAP].astype(jnp.int32)


def with_ends(entries, own_key, least, top_value):
    longest = entries.shape.index(max(entries.shape))
    spots = []
    for shift in (0, 1):
        where = [jax.random.randint(jax.random.fold_in(own_key, axis), (), 0, length) for axis, length in enumerate(entries.shape)]
        where[longest] = (where[longest] + shift) % entries.shape[longest]
        spots.append(tuple(where))
    return entries.at[spots[0]].set(least).at[spots[1]].set(top_value)


def steps_of(stream_key, shape, cuts, low, high):
    def one(position, blocks):
        draws = jax.random.uniform(jax.random.fold_in(jax.random.fold_in(stream_key, 6), position), (blocks,), jnp.float32, low / len(cuts), high / len(cuts))
        return jnp.repeat(jnp.exp(draws), shape[position] // blocks).reshape((-1,) + (1,) * (len(shape) - position - 1))

    factor_of = one(*cuts[0])
    for cut in cuts[1:]:
        factor_of = factor_of * one(*cut)
    return factor_of


def gaussian(own_key, extent, spread, most, pieces=(), kind=jnp.bfloat16):
    gain = steps_of(own_key, extent, pieces, -0.22, 0.18) if pieces else 1.0
    entries = jax.random.normal(own_key, extent, jnp.float32) * spread * gain
    return jnp.minimum(jnp.maximum(entries, -most), most).astype(kind)


def setup_inputs(seed: int = 0) -> dict:
    splits = jax.random.split(jax.random.key(seed), 12)
    positions = gaussian(splits[0], (3, NODES), 1.0, 6.0, ((1, 32),), jnp.float32)
    densities = gaussian(splits[1], (3, NODES), 1.0, 6.0, ((1, 32),), jnp.float32)
    near_src = draw_near_src(jax.random.fold_in(splits[11], 71), 0)
    near_count = draw_near_count(jax.random.fold_in(splits[11], 71), 0)
    far_slot = with_ends(jax.random.randint(splits[4], (LEAVES, FAR), 0, SLOTS), jax.random.fold_in(splits[4], 1), 0, SLOTS - 1).astype(jnp.int32)
    far_class = with_ends(jax.random.randint(splits[5], (LEAVES, FAR), 0, CLASSES), jax.random.fold_in(splits[5], 1), 0, CLASSES - 1).astype(jnp.int32)
    far_count = with_ends(jax.random.randint(splits[6], (LEAVES,), 1, FAR + 1), jax.random.fold_in(splits[6], 1), 1, FAR).astype(jnp.int32)
    requests = draw_requests(jax.random.fold_in(splits[11], 71), 0)
    up_basis = gaussian(splits[8], (LEAVES, 3 * RANK, 3 * P_SIZE), (3 * P_SIZE) ** -0.5, 0.3125, ((0, 32),))
    transfer_table = gaussian(splits[9], (CLASSES, 9 * RANK * RANK), (3 * RANK) ** -0.5, 0.5)
    down_basis = gaussian(splits[10], (LEAVES, 3 * RANK, 9, P_SIZE), (3 * RANK * FAR) ** -0.5, 0.09375, ((0, 32),))
    return dict(positions=positions, densities=densities, near_src=near_src, near_count=near_count, far_slot=far_slot, far_class=far_class, far_count=far_count, requests=requests, up_basis=up_basis, transfer_table=transfer_table, down_basis=down_basis)


KERNEL = 1.0 / (8.0 * math.pi)
BLOB = 0.25

def pair_terms(target, source):
    xt = target[:, :3]
    ft = target[:, 3:]
    xs = source[:, :3]
    fs = source[:, 3:]
    sep = xt[:, :, :, None] - xs[:, :, None, :]
    rho_sq = lax.optimization_barrier(jnp.sum(sep * sep, axis=1)) + BLOB
    inv_one = lax.rsqrt(rho_sq)
    inv_three = inv_one / rho_sq
    inv_five = inv_three / rho_sq
    fa = ft[:, :, :, None]
    fb = fs[:, :, None, :]
    prod_ab = lax.optimization_barrier(jnp.sum(fa * fb, axis=1))
    prod_ar = lax.optimization_barrier(jnp.sum(fa * sep, axis=1))
    prod_br = lax.optimization_barrier(jnp.sum(fb * sep, axis=1))
    first = (fa * prod_br[:, None] + fb * prod_ar[:, None] - prod_ab[:, None] * sep) * inv_three[:, None]
    second = 3.0 * (prod_ar * prod_br * inv_five)[:, None] * sep
    return (first - second) * KERNEL

def reference(positions, densities, near_src, near_count, far_slot, far_class, far_count, requests, up_basis, transfer_table, down_basis):
    stacked = jnp.concatenate([positions, densities], 0).reshape(6, LEAVES, P_SIZE).transpose(1, 0, 2)
    blocks = jnp.arange(N_PATCH, dtype=jnp.int32)

    def slot_body(slot, grad):
        source = near_src[:, slot]
        live = (slot < near_count).astype(jnp.float32)

        def one_block(block):
            start = (block * LEAF_DEV).astype(jnp.int32)
            target = lax.dynamic_slice_in_dim(stacked, start, LEAF_DEV, 0)
            src_ids = lax.dynamic_slice_in_dim(source, start, LEAF_DEV, 0)
            weight = lax.dynamic_slice_in_dim(live, start, LEAF_DEV, 0)
            terms = pair_terms(target, stacked[src_ids]) * weight[:, None, None, None]
            return (lax.optimization_barrier(jnp.sum(terms, axis=3)), lax.optimization_barrier(jnp.sum(terms, axis=2)))
        tgt_sum, src_sum = lax.map(one_block, blocks)
        grad = grad + tgt_sum.reshape(LEAVES, 3, P_SIZE)
        return grad.at[source].add(-src_sum.reshape(LEAVES, 3, P_SIZE))
    near = lax.fori_loop(0, NEAR, slot_body, jnp.zeros((LEAVES, 3, P_SIZE), jnp.float32))
    dens_leaf = stacked[:, 3:]
    dens_round = lax.optimization_barrier(dens_leaf.reshape(LEAVES, 3 * P_SIZE).astype(jnp.bfloat16))
    dens_flat = dens_round.astype(jnp.float32)

    def upward(block):
        start = (block * LEAF_DEV).astype(jnp.int32)
        basis = lax.dynamic_slice_in_dim(up_basis, start, LEAF_DEV, 0).astype(jnp.float32)
        dens_b = lax.dynamic_slice_in_dim(dens_flat, start, LEAF_DEV, 0)
        return jnp.einsum('lrq,lq->lr', basis, dens_b, precision=lax.Precision.HIGHEST).astype(jnp.bfloat16)
    moments = lax.map(upward, blocks).reshape(LEAVES, 3 * RANK)
    moments = lax.optimization_barrier(moments).astype(jnp.float32)
    dev_of = jnp.arange(LEAVES, dtype=jnp.int32) // LEAF_DEV
    peer = far_slot // CAP
    place = far_slot % CAP
    source_ids = peer * LEAF_DEV + requests[dev_of[:, None], peer, place]

    def far_block(block):
        start = (block * LEAF_DEV).astype(jnp.int32)
        ids = lax.dynamic_slice_in_dim(source_ids, start, LEAF_DEV, 0)
        classes = lax.dynamic_slice_in_dim(far_class, start, LEAF_DEV, 0)
        counts = lax.dynamic_slice_in_dim(far_count, start, LEAF_DEV, 0)

        def far_step(slot, expansion):
            src = moments[ids[:, slot]]
            oper = transfer_table[classes[:, slot]].reshape(LEAF_DEV, 3 * RANK, 3 * RANK).astype(jnp.float32)
            live = (slot < counts).astype(jnp.float32)
            return expansion + live[:, None] * jnp.einsum('lij,lj->li', oper, src, precision=lax.Precision.HIGHEST)
        expansion = lax.fori_loop(0, FAR, far_step, jnp.zeros((LEAF_DEV, 3 * RANK), jnp.float32))
        expansion = lax.optimization_barrier(expansion.astype(jnp.bfloat16)).astype(jnp.float32)
        basis = lax.dynamic_slice_in_dim(down_basis, start, LEAF_DEV, 0).astype(jnp.float32)
        field = jnp.einsum('lr,lrqp->lqp', expansion, basis, precision=lax.Precision.HIGHEST)
        dens_b = lax.dynamic_slice_in_dim(dens_leaf, start, LEAF_DEV, 0)
        return jnp.einsum('lcp,lckp->lkp', dens_b, field.reshape(LEAF_DEV, 3, 3, P_SIZE), precision=lax.Precision.HIGHEST)
    far = lax.map(far_block, blocks).reshape(LEAVES, 3, P_SIZE)
    return (near + far).transpose(1, 0, 2).reshape(3, NODES)
```

```python
import functools
import math

import jax
import jax.numpy as jnp
from jax import lax
from jax.experimental import pallas as pl
from jax.experimental.pallas import tpu as pltpu
from jax.sharding import PartitionSpec as P

KERNEL = 1.0 / (8.0 * math.pi)
BLOB = 0.25
MESH = pl.DeviceIdType.MESH
F32 = jnp.float32
BF16 = jnp.bfloat16


def iota(shape, dim):
    return lax.broadcasted_iota(jnp.int32, shape, dim)


def dot(a, b):
    return jnp.dot(a, b, preferred_element_type=F32)


def exchange(
    n,
    pos,
    dens,
    up_hbm,
    pos_b,
    pos_a,
    dens_b,
    dens_a,
    mom,
    up,
    dens_rows,
    local_sem,
    halo_send,
    halo_recv,
    mom_send,
    mom_recv,
):
    leaves, width = mom.shape[1:]
    size = pos.shape[1] // leaves
    me = lax.axis_index("patch")
    right = lax.rem(me + 1, n)
    left = lax.rem(me + n - 1, n)
    get_up = pltpu.make_async_copy(up_hbm, up, local_sem)
    get_up.start()
    barrier = pltpu.get_barrier_semaphore()

    @pl.loop(1, n)
    def _(k):
        pl.semaphore_signal(
            barrier, inc=1, device_id=(lax.rem(me + k, n),), device_id_type=MESH
        )

    for leaf in range(leaves):
        for c in range(3):
            dens_rows[leaf : leaf + 1, c * size : (c + 1) * size] = dens[
                c : c + 1, leaf * size : (leaf + 1) * size
            ]
    dens_round = dens_rows[...].astype(BF16)
    get_up.wait()
    row = iota((leaves, width), 0)
    total = jnp.zeros((leaves, width), F32)
    for leaf in range(leaves):
        got = lax.dot_general(
            dens_round, up[leaf], (((1,), (1,)), ((), ())), preferred_element_type=F32
        )
        total = total + jnp.where(row == leaf, got, 0.0)
    mom[me] = total.astype(BF16)

    pl.semaphore_wait(barrier, n - 1)
    halos = []
    for k, (src, dst, peer) in enumerate(
        ((pos, pos_b, right), (dens, dens_b, right), (pos, pos_a, left), (dens, dens_a, left))
    ):
        copy = pltpu.make_async_remote_copy(
            src_ref=src,
            dst_ref=dst,
            send_sem=halo_send.at[k],
            recv_sem=halo_recv.at[k],
            device_id=(peer,),
            device_id_type=MESH,
        )
        copy.start()
        halos.append(copy)

    def mom_copy(k):
        return pltpu.make_async_remote_copy(
            src_ref=mom.at[me],
            dst_ref=mom.at[me],
            send_sem=mom_send.at[k],
            recv_sem=mom_recv.at[k],
            device_id=(lax.rem(me + k, n),),
            device_id_type=MESH,
        )

    @pl.loop(1, n)
    def _(k):
        mom_copy(k).start()

    for copy in halos:
        copy.wait_recv()

    @pl.loop(1, n)
    def _(k):
        mom_copy(k).wait_recv()

    for copy in halos:
        copy.wait_send()

    @pl.loop(1, n)
    def _(k):
        mom_copy(k).wait_send()


def near_field(
    near_src,
    near_count,
    first,
    pos,
    dens,
    pos_b,
    pos_a,
    dens_b,
    dens_a,
    near,
    part_b,
    part_a,
    window,
    tb,
    tacc,
    near_t,
    src_acc,
):
    leaves = near_count.shape[0]
    size = pos.shape[1] // leaves
    src_acc[...] = jnp.zeros_like(src_acc)
    window[...] = jnp.zeros_like(window)
    for part, (x, f) in enumerate(((pos_b, dens_b), (pos, dens), (pos_a, dens_a))):
        for leaf in range(leaves):
            lanes = slice(leaf * size, (leaf + 1) * size)
            window[part * leaves + leaf, 0:3, :] = x[:, lanes]
            window[part * leaves + leaf, 3:6, :] = f[:, lanes]

    offset = first[0]
    lane = iota((size, size), 1)

    @pl.loop(0, leaves)
    def _(leaf):
        columns = jnp.transpose(window[leaves + leaf])
        for c in range(6):
            col = columns[:, c : c + 1]
            if c >= 3:
                col = col * KERNEL
            tb[c] = jnp.broadcast_to(col, (size, size))
        tacc[...] = jnp.zeros_like(tacc)

        def near_block(slot, carry):
            index = near_src[slot, leaf] - offset
            other = window[index]
            xs = [jnp.broadcast_to(other[c : c + 1], (8, size)) for c in range(3)]
            fs = [jnp.broadcast_to(other[c : c + 1], (8, size)) for c in range(3, 6)]
            src_sum = [None] * 3
            for g in range(size // 8):
                r8 = slice(g * 8, (g + 1) * 8)
                ft = [tb[3 + c, r8, :] for c in range(3)]
                sep = [tb[c, r8, :] - xs[c] for c in range(3)]
                rho = sep[0] * sep[0] + sep[1] * sep[1] + sep[2] * sep[2] + BLOB
                inv1 = lax.rsqrt(rho)
                inv2 = inv1 * inv1
                inv3 = inv1 * inv2
                ab = ft[0] * fs[0] + ft[1] * fs[1] + ft[2] * fs[2]
                ar = ft[0] * sep[0] + ft[1] * sep[1] + ft[2] * sep[2]
                br = fs[0] * sep[0] + fs[1] * sep[1] + fs[2] * sep[2]
                p = br * inv3
                q = ar * inv3
                w = ab * inv3 + (3.0 * (p * ar)) * inv2
                for c in range(3):
                    t = ft[c] * p + fs[c] * q - w * sep[c]
                    tacc[c, r8, :] += t
                    src_sum[c] = t if g == 0 else src_sum[c] + t
            for c in range(3):
                src_acc[index, c] += src_sum[c]
            return carry

        lax.fori_loop(0, near_count[leaf], near_block, 0)
        cols = [jnp.sum(tacc[c], axis=1, keepdims=True) for c in range(3)]
        mixed = jnp.where(lane == 0, cols[0], jnp.where(lane == 1, cols[1], cols[2]))
        near_t[leaf] = jnp.transpose(mixed)[0:8]

    for part, buf in ((0, part_b), (2, part_a)):
        for leaf in range(leaves):
            for c in range(3):
                buf[c : c + 1, leaf * size : (leaf + 1) * size] = jnp.sum(
                    src_acc[part * leaves + leaf, c], axis=0, keepdims=True
                )
    for leaf in range(leaves):
        for c in range(3):
            near[c : c + 1, leaf * size : (leaf + 1) * size] = near_t[
                leaf, c : c + 1, :
            ] - jnp.sum(src_acc[leaves + leaf, c], axis=0, keepdims=True)


def far_field(
    far_count,
    dens,
    far_slot,
    far_class,
    req,
    mom,
    table_hbm,
    down_hbm,
    far_out,
    table,
    down,
    hot_class,
    hot_slot,
    tiled,
    sums,
    fold,
    expan,
    far_acc,
    table_sem,
    down_sem,
):
    n, leaves, width = mom.shape
    size = dens.shape[1] // leaves
    far_num = far_slot.shape[1]
    classes = table.shape[0]
    cap = req.shape[1]
    block = fold.shape[0]

    def table_copy(b):
        lanes = pl.ds(pl.multiple_of(b * block, 128), block)
        return pltpu.make_async_copy(
            table_hbm.at[:, lanes], table.at[:, lanes], table_sem.at[b]
        )

    for b in range(width * width // block):
        table_copy(b).start()
    get_down = pltpu.make_async_copy(down_hbm, down, down_sem)
    get_down.start()
    count_col = jnp.zeros((leaves, 1), jnp.int32)
    leaf_col = iota((leaves, 1), 0)
    for leaf in range(leaves):
        count_col = jnp.where(leaf_col == leaf, far_count[leaf], count_col)
    class_iota = iota((leaves, classes), 1)
    dev_iota = iota((leaves, n), 1) * cap
    for s in range(far_num):
        rows = slice(s * leaves, (s + 1) * leaves)
        wanted = jnp.where(s < count_col, far_class[:, s : s + 1], -1)
        hot_class[rows, :] = (class_iota == wanted).astype(F32).astype(BF16)
        slot = far_slot[:, s : s + 1]
        for place in range(cap):
            hot_slot[place, rows, :] = (dev_iota + place == slot).astype(F32).astype(BF16)
    fold_row = iota(fold.shape, 0)
    fold_first = iota(fold.shape, 1) * width
    fold[...] = (
        ((fold_row >= fold_first) & (fold_row < fold_first + width)).astype(F32).astype(BF16)
    )
    period = tiled.shape[1]
    spread_gap = iota((width, period), 1) - iota((width, period), 0)
    spread = spread_gap == 0
    for k in range(1, period // width):
        spread = spread | (spread_gap == k * width)
    spread = spread.astype(F32).astype(BF16)
    moments = mom[...].reshape(n * leaves, width)
    leaf_iota = iota((n, n * leaves), 1) - iota((n, n * leaves), 0) * leaves
    picked = []
    for place in range(cap):
        pick = (leaf_iota == req[:, place : place + 1]).astype(F32).astype(BF16)
        chosen = dot(pick, moments).astype(BF16)
        picked.append(dot(chosen, spread).astype(BF16))
    for k in range(period // 128):
        lanes = slice(k * 128, (k + 1) * 128)
        acc = dot(hot_slot[0], picked[0][:, lanes])
        for place in range(1, cap):
            acc = acc + dot(hot_slot[place], picked[place][:, lanes])
        tiled[:, lanes] = acc

    expan[...] = jnp.zeros_like(expan)
    step = 256 if block % 256 == 0 else 128
    per_block = block // width

    @pl.loop(0, width * width // block)
    def _(b):
        table_copy(b).wait()
        for t in range(block // step):
            start = pl.multiple_of(b * block + t * step, 128)
            oper = dot(hot_class[...], table[:, pl.ds(start, step)])
            for h in range(step // 128):
                at = ((t * step) // 128 + h) % (period // 128)
                acc = None
                for s in range(far_num):
                    rows = slice(s * leaves, (s + 1) * leaves)
                    term = oper[rows, h * 128 : (h + 1) * 128] * tiled[
                        rows, at * 128 : (at + 1) * 128
                    ]
                    acc = term if acc is None else acc + term
                sums[:, t * step + h * 128 : t * step + (h + 1) * 128] = acc
        whole = sums[...]
        high = whole.astype(BF16)
        low = (whole - high.astype(F32)).astype(BF16)
        res = dot(high, fold[...]) + dot(low, fold[...])
        wide = jnp.concatenate([res, jnp.zeros((leaves, expan.shape[1] - 128), F32)], axis=1)
        expan[...] += pltpu.roll(wide, b * per_block, 1)

    expansion = expan[...][:, :width].astype(BF16)
    get_down.wait()
    far_acc[...] = jnp.zeros_like(far_acc)
    leaf_row = iota((leaves, size), 0)

    @pl.loop(0, leaves)
    def _(leaf):
        lanes = pl.ds(pl.multiple_of(leaf * size, size), size)
        own = dens[:, lanes]
        fields = [dot(expansion, down[leaf, q]) for q in range(9)]
        for k in range(3):
            far = (
                own[0:1] * fields[k] + own[1:2] * fields[3 + k] + own[2:3] * fields[6 + k]
            )
            far_acc[k] += jnp.where(leaf_row == leaf, far, 0.0)

    for leaf in range(leaves):
        for c in range(3):
            far_out[c : c + 1, leaf * size : (leaf + 1) * size] = far_acc[
                c, leaf : leaf + 1, :
            ]


def per_device(
    n,
    positions,
    densities,
    near_src,
    near_count,
    far_slot,
    far_class,
    far_count,
    requests,
    up_basis,
    transfer_table,
    down_basis,
):
    leaves = near_count.shape[0]
    nodes = positions.shape[1]
    size = nodes // leaves
    width = up_basis.shape[1]
    far_num = far_slot.shape[1]
    cap = requests.shape[2]
    classes = transfer_table.shape[0]
    period = math.lcm(width, 128)
    blocks = width * width // period
    block = 2 * period if blocks % 2 == 0 else period
    down = jnp.transpose(down_basis, (0, 2, 1, 3))
    blocks = width * width // block
    smem = pl.BlockSpec(memory_space=pltpu.SMEM)
    vmem = pl.BlockSpec(memory_space=pltpu.VMEM)
    hbm = pl.BlockSpec(memory_space=pl.ANY)
    line = jax.ShapeDtypeStruct((3, nodes), F32)
    limit = 60 * 1024 * 1024
    pos_b, pos_a, dens_b, dens_a, mom = pl.pallas_call(
        functools.partial(exchange, n),
        out_shape=[line] * 4 + [jax.ShapeDtypeStruct((n, leaves, width), BF16)],
        in_specs=[vmem] * 2 + [hbm],
        out_specs=[vmem] * 5,
        scratch_shapes=[
            pltpu.VMEM(up_basis.shape, BF16),
            pltpu.VMEM((leaves, 3 * size), F32),
            pltpu.SemaphoreType.DMA,
            pltpu.SemaphoreType.DMA((4,)),
            pltpu.SemaphoreType.DMA((4,)),
            pltpu.SemaphoreType.DMA((n,)),
            pltpu.SemaphoreType.DMA((n,)),
        ],
        compiler_params=pltpu.CompilerParams(
            collective_id=0, has_side_effects=True, vmem_limit_bytes=limit
        ),
    )(positions, densities, up_basis)
    first = ((lax.axis_index("patch") - 1) * leaves).reshape(1)
    near, part_b, part_a = pl.pallas_call(
        near_field,
        out_shape=[line] * 3,
        in_specs=[smem] * 3 + [vmem] * 6,
        out_specs=[vmem] * 3,
        scratch_shapes=[
            pltpu.VMEM((3 * leaves, 8, size), F32),
            pltpu.VMEM((6, size, size), F32),
            pltpu.VMEM((3, size, size), F32),
            pltpu.VMEM((leaves, 8, size), F32),
            pltpu.VMEM((3 * leaves, 3, 8, size), F32),
        ],
        compiler_params=pltpu.CompilerParams(vmem_limit_bytes=limit),
    )(near_src.T, near_count, first, positions, densities, pos_b, pos_a, dens_b, dens_a)
    up_pairs = [(i, i + 1) for i in range(n - 1)]
    got_a = lax.ppermute(part_b, "patch", [(j, i) for i, j in up_pairs])
    got_b = lax.ppermute(part_a, "patch", up_pairs)
    far = pl.pallas_call(
        far_field,
        out_shape=line,
        in_specs=[smem] + [vmem] * 5 + [hbm] * 2,
        out_specs=vmem,
        scratch_shapes=[
            pltpu.VMEM(transfer_table.shape, BF16),
            pltpu.VMEM(down.shape, BF16),
            pltpu.VMEM((far_num * leaves, classes), BF16),
            pltpu.VMEM((cap, far_num * leaves, n), BF16),
            pltpu.VMEM((far_num * leaves, period), F32),
            pltpu.VMEM((leaves, block), F32),
            pltpu.VMEM((block, 128), BF16),
            pltpu.VMEM((leaves, (width + 127) // 128 * 128), F32),
            pltpu.VMEM((3, leaves, size), F32),
            pltpu.SemaphoreType.DMA((blocks,)),
            pltpu.SemaphoreType.DMA,
        ],
        cost_estimate=pl.CostEstimate(
            flops=2 * far_num * leaves * 256 * width * width,
            bytes_accessed=2 * (transfer_table.size + down.size),
            transcendentals=0,
        ),
        compiler_params=pltpu.CompilerParams(vmem_limit_bytes=limit),
    )(far_count, densities, far_slot, far_class, requests[0], mom, transfer_table, down)
    return near + far - got_a - got_b


def solution(mesh):
    placed = (
        P(None, "patch"),
        P(None, "patch"),
        P("patch", None),
        P("patch"),
        P("patch", None),
        P("patch", None),
        P("patch"),
        P("patch", None, None),
        P("patch", None, None),
        P(),
        P("patch", None, None, None),
    )
    return jax.shard_map(
        functools.partial(per_device, mesh.shape["patch"]),
        mesh=mesh,
        in_specs=placed,
        out_specs=P(None, "patch"),
        check_vma=False,
    )
```

```python
import functools
import math

import jax
import jax.numpy as jnp
from jax import lax
from jax.experimental import pallas as pl
from jax.experimental.pallas import tpu as pltpu
from jax.sharding import PartitionSpec as P

KERNEL = 1.0 / (8.0 * math.pi)
BLOB = 0.25
MESH = pl.DeviceIdType.MESH
F32 = jnp.float32
BF16 = jnp.bfloat16


def iota(shape, dim):
    return lax.broadcasted_iota(jnp.int32, shape, dim)


def dot(a, b):
    return jnp.dot(a, b, preferred_element_type=F32)


def exchange(
    n,
    pos,
    dens,
    up_hbm,
    pos_b,
    pos_a,
    dens_b,
    dens_a,
    mom,
    up,
    dens_rows,
    local_sem,
    halo_send,
    halo_recv,
):
    leaves, width = mom.shape
    size = pos.shape[1] // leaves
    me = lax.axis_index("patch")
    right = lax.rem(me + 1, n)
    left = lax.rem(me + n - 1, n)
    get_up = pltpu.make_async_copy(up_hbm, up, local_sem)
    get_up.start()
    barrier = pltpu.get_barrier_semaphore()

    for peer in (left, right):
        pl.semaphore_signal(barrier, inc=1, device_id=(peer,), device_id_type=MESH)

    for leaf in range(leaves):
        for c in range(3):
            dens_rows[leaf : leaf + 1, c * size : (c + 1) * size] = dens[
                c : c + 1, leaf * size : (leaf + 1) * size
            ]
    dens_round = dens_rows[...].astype(BF16)
    pl.semaphore_wait(barrier, 2)
    halos = []
    for k, (src, dst, peer) in enumerate(
        ((pos, pos_b, right), (dens, dens_b, right), (pos, pos_a, left), (dens, dens_a, left))
    ):
        copy = pltpu.make_async_remote_copy(
            src_ref=src,
            dst_ref=dst,
            send_sem=halo_send.at[k],
            recv_sem=halo_recv.at[k],
            device_id=(peer,),
            device_id_type=MESH,
        )
        copy.start()
        halos.append(copy)

    get_up.wait()
    row = iota((leaves, width), 0)
    total = jnp.zeros((leaves, width), F32)
    for leaf in range(leaves):
        got = lax.dot_general(
            dens_round, up[leaf], (((1,), (1,)), ((), ())), preferred_element_type=F32
        )
        total = total + jnp.where(row == leaf, got, 0.0)
    mom[...] = total.astype(BF16)

    for copy in halos:
        copy.wait()


def near_field(
    near_src,
    near_count,
    first,
    pos,
    dens,
    pos_b,
    pos_a,
    dens_b,
    dens_a,
    near,
    part_b,
    part_a,
    window,
    tb,
    tacc,
    near_t,
    src_acc,
):
    leaves = near_count.shape[0]
    size = pos.shape[1] // leaves
    src_acc[...] = jnp.zeros_like(src_acc)
    window[...] = jnp.zeros_like(window)
    for part, (x, f) in enumerate(((pos_b, dens_b), (pos, dens), (pos_a, dens_a))):
        for leaf in range(leaves):
            lanes = slice(leaf * size, (leaf + 1) * size)
            window[part * leaves + leaf, 0:3, :] = x[:, lanes]
            window[part * leaves + leaf, 3:6, :] = f[:, lanes]

    offset = first[0]
    lane = iota((size, size), 1)

    @pl.loop(0, leaves)
    def _(leaf):
        columns = jnp.transpose(window[leaves + leaf])
        for c in range(6):
            col = columns[:, c : c + 1]
            if c >= 3:
                col = col * KERNEL
            tb[c] = jnp.broadcast_to(col, (size, size))
        tacc[...] = jnp.zeros_like(tacc)

        def near_block(slot, carry):
            index = near_src[slot, leaf] - offset
            other = window[index]
            xs = [jnp.broadcast_to(other[c : c + 1], (8, size)) for c in range(3)]
            fs = [jnp.broadcast_to(other[c : c + 1], (8, size)) for c in range(3, 6)]
            src_sum = [None] * 3
            for g in range(size // 8):
                r8 = slice(g * 8, (g + 1) * 8)
                ft = [tb[3 + c, r8, :] for c in range(3)]
                sep = [tb[c, r8, :] - xs[c] for c in range(3)]
                rho = sep[0] * sep[0] + sep[1] * sep[1] + sep[2] * sep[2] + BLOB
                inv1 = lax.rsqrt(rho)
                inv2 = inv1 * inv1
                inv3 = inv1 * inv2
                ab = ft[0] * fs[0] + ft[1] * fs[1] + ft[2] * fs[2]
                ar = ft[0] * sep[0] + ft[1] * sep[1] + ft[2] * sep[2]
                br = fs[0] * sep[0] + fs[1] * sep[1] + fs[2] * sep[2]
                p = br * inv3
                q = ar * inv3
                w = ab * inv3 + (3.0 * (p * ar)) * inv2
                for c in range(3):
                    t = ft[c] * p + fs[c] * q - w * sep[c]
                    tacc[c, r8, :] += t
                    src_sum[c] = t if g == 0 else src_sum[c] + t
            for c in range(3):
                src_acc[index, c] += src_sum[c]
            return carry

        lax.fori_loop(0, near_count[leaf], near_block, 0)
        cols = [jnp.sum(tacc[c], axis=1, keepdims=True) for c in range(3)]
        mixed = jnp.where(lane == 0, cols[0], jnp.where(lane == 1, cols[1], cols[2]))
        near_t[leaf] = jnp.transpose(mixed)[0:8]

    for part, buf in ((0, part_b), (2, part_a)):
        for leaf in range(leaves):
            for c in range(3):
                buf[c : c + 1, leaf * size : (leaf + 1) * size] = jnp.sum(
                    src_acc[part * leaves + leaf, c], axis=0, keepdims=True
                )
    for leaf in range(leaves):
        for c in range(3):
            near[c : c + 1, leaf * size : (leaf + 1) * size] = near_t[
                leaf, c : c + 1, :
            ] - jnp.sum(src_acc[leaves + leaf, c], axis=0, keepdims=True)


def far_field(
    n,
    far_count,
    dens,
    far_slot,
    far_class,
    req,
    mom_own,
    near,
    part_b,
    part_a,
    table_hbm,
    down_hbm,
    out,
    mom,
    got_b,
    got_a,
    table,
    down,
    hot_class,
    hot_slot,
    tiled,
    sums,
    fold,
    expan,
    far_acc,
    table_sem,
    down_sem,
    mom_send,
    mom_recv,
    part_send,
    part_recv,
):
    leaves, width = mom_own.shape
    me = lax.axis_index("patch")
    barrier = pltpu.get_barrier_semaphore()

    @pl.loop(1, n)
    def _(k):
        pl.semaphore_signal(
            barrier, inc=1, device_id=(lax.rem(me + k, n),), device_id_type=MESH
        )

    size = dens.shape[1] // leaves
    far_num = far_slot.shape[1]
    classes = table.shape[0]
    cap = req.shape[0]
    block = fold.shape[0]

    def table_copy(b):
        lanes = pl.ds(pl.multiple_of(b * block, 128), block)
        return pltpu.make_async_copy(
            table_hbm.at[:, lanes], table.at[:, lanes], table_sem.at[b]
        )

    for b in range(width * width // block):
        table_copy(b).start()
    get_down = pltpu.make_async_copy(down_hbm, down, down_sem)
    get_down.start()
    count_col = jnp.zeros((leaves, 1), jnp.int32)
    leaf_col = iota((leaves, 1), 0)
    for leaf in range(leaves):
        count_col = jnp.where(leaf_col == leaf, far_count[leaf], count_col)
    class_iota = iota((leaves, classes), 1)
    for s in range(far_num):
        rows = slice(s * leaves, (s + 1) * leaves)
        wanted = jnp.where(s < count_col, far_class[:, s : s + 1], -1)
        hot_class[rows, :] = (class_iota == wanted).astype(F32).astype(BF16)
    fold_row = iota(fold.shape, 0)
    fold_first = iota(fold.shape, 1) * width
    fold[...] = (
        ((fold_row >= fold_first) & (fold_row < fold_first + width)).astype(F32).astype(BF16)
    )
    pl.semaphore_wait(barrier, n - 1)

    def mom_copy(k):
        return pltpu.make_async_remote_copy(
            src_ref=mom_own,
            dst_ref=mom.at[me],
            send_sem=mom_send.at[k],
            recv_sem=mom_recv.at[k],
            device_id=(lax.rem(me + k, n),),
            device_id_type=MESH,
        )

    @pl.loop(1, n)
    def _(k):
        mom_copy(k).start()

    parts = []
    for k, (src, dst, peer) in enumerate(
        (
            (part_b, got_a, lax.rem(me + n - 1, n)),
            (part_a, got_b, lax.rem(me + 1, n)),
        )
    ):
        copy = pltpu.make_async_remote_copy(
            src_ref=src,
            dst_ref=dst,
            send_sem=part_send.at[k],
            recv_sem=part_recv.at[k],
            device_id=(peer,),
            device_id_type=MESH,
        )
        copy.start()
        parts.append(copy)

    mom[me] = mom_own[...]
    dev_iota = iota((leaves, n), 1) * cap
    for s in range(far_num):
        rows = slice(s * leaves, (s + 1) * leaves)
        slot = far_slot[:, s : s + 1]
        for place in range(cap):
            hot_slot[place, rows, :] = (dev_iota + place == slot).astype(F32).astype(BF16)
    period = tiled.shape[1]
    spread_gap = iota((width, period), 1) - iota((width, period), 0)
    spread = spread_gap == 0
    for k in range(1, period // width):
        spread = spread | (spread_gap == k * width)
    spread = spread.astype(F32).astype(BF16)

    @pl.loop(1, n)
    def _(k):
        mom_copy(k).wait_recv()

    moments = mom[...].reshape(n * leaves, width)
    leaf_iota = iota((n * leaves, n), 0) - iota((n * leaves, n), 1) * leaves
    picked = []
    for place in range(cap):
        pick = (leaf_iota == req[place : place + 1, :]).astype(F32).astype(BF16)
        chosen = lax.dot_general(
            pick, moments, (((0,), (0,)), ((), ())), preferred_element_type=F32
        ).astype(BF16)
        picked.append(dot(chosen, spread).astype(BF16))
    for k in range(period // 128):
        lanes = slice(k * 128, (k + 1) * 128)
        acc = dot(hot_slot[0], picked[0][:, lanes])
        for place in range(1, cap):
            acc = acc + dot(hot_slot[place], picked[place][:, lanes])
        tiled[:, lanes] = acc

    expan[...] = jnp.zeros_like(expan)
    step = 256 if block % 256 == 0 else 128
    per_block = block // width

    @pl.loop(0, width * width // block)
    def _(b):
        table_copy(b).wait()
        for t in range(block // step):
            start = pl.multiple_of(b * block + t * step, 128)
            oper = dot(hot_class[...], table[:, pl.ds(start, step)])
            for h in range(step // 128):
                at = ((t * step) // 128 + h) % (period // 128)
                acc = None
                for s in range(far_num):
                    rows = slice(s * leaves, (s + 1) * leaves)
                    term = oper[rows, h * 128 : (h + 1) * 128] * tiled[
                        rows, at * 128 : (at + 1) * 128
                    ]
                    acc = term if acc is None else acc + term
                sums[:, t * step + h * 128 : t * step + (h + 1) * 128] = acc
        whole = sums[...]
        high = whole.astype(BF16)
        low = (whole - high.astype(F32)).astype(BF16)
        res = dot(high, fold[...]) + dot(low, fold[...])
        wide = jnp.concatenate([res, jnp.zeros((leaves, expan.shape[1] - 128), F32)], axis=1)
        expan[...] += pltpu.roll(wide, b * per_block, 1)

    expansion = expan[...][:, :width].astype(BF16)
    get_down.wait()
    far_acc[...] = jnp.zeros_like(far_acc)
    leaf_row = iota((leaves, size), 0)

    @pl.loop(0, leaves)
    def _(leaf):
        lanes = pl.ds(pl.multiple_of(leaf * size, size), size)
        own = dens[:, lanes]
        fields = [dot(expansion, down[leaf, q]) for q in range(9)]
        for k in range(3):
            far = (
                own[0:1] * fields[k] + own[1:2] * fields[3 + k] + own[2:3] * fields[6 + k]
            )
            far_acc[k] += jnp.where(leaf_row == leaf, far, 0.0)

    for copy in parts:
        copy.wait_recv()
    for leaf in range(leaves):
        lanes = slice(leaf * size, (leaf + 1) * size)
        for c in range(3):
            came = got_b[c : c + 1, lanes] + got_a[c : c + 1, lanes]
            out[c : c + 1, lanes] = near[c : c + 1, lanes] - came + far_acc[c, leaf : leaf + 1, :]
    for copy in parts:
        copy.wait_send()

    @pl.loop(1, n)
    def _(k):
        mom_copy(k).wait_send()


def per_device(
    n,
    positions,
    densities,
    near_src,
    near_count,
    far_slot,
    far_class,
    far_count,
    requests,
    up_basis,
    transfer_table,
    down_basis,
):
    leaves = near_count.shape[0]
    nodes = positions.shape[1]
    size = nodes // leaves
    width = up_basis.shape[1]
    far_num = far_slot.shape[1]
    cap = requests.shape[2]
    classes = transfer_table.shape[0]
    period = math.lcm(width, 128)
    blocks = width * width // period
    block = 2 * period if blocks % 2 == 0 else period
    down = jnp.transpose(down_basis, (0, 2, 1, 3))
    blocks = width * width // block
    smem = pl.BlockSpec(memory_space=pltpu.SMEM)
    vmem = pl.BlockSpec(memory_space=pltpu.VMEM)
    hbm = pl.BlockSpec(memory_space=pl.ANY)
    line = jax.ShapeDtypeStruct((3, nodes), F32)
    limit = 60 * 1024 * 1024
    pos_b, pos_a, dens_b, dens_a, mom = pl.pallas_call(
        functools.partial(exchange, n),
        out_shape=[line] * 4 + [jax.ShapeDtypeStruct((leaves, width), BF16)],
        in_specs=[vmem] * 2 + [hbm],
        out_specs=[vmem] * 5,
        scratch_shapes=[
            pltpu.VMEM(up_basis.shape, BF16),
            pltpu.VMEM((leaves, 3 * size), F32),
            pltpu.SemaphoreType.DMA,
            pltpu.SemaphoreType.DMA((4,)),
            pltpu.SemaphoreType.DMA((4,)),
        ],
        compiler_params=pltpu.CompilerParams(
            collective_id=0, has_side_effects=True, vmem_limit_bytes=limit
        ),
    )(positions, densities, up_basis)
    first = ((lax.axis_index("patch") - 1) * leaves).reshape(1)
    near, part_b, part_a = pl.pallas_call(
        near_field,
        out_shape=[line] * 3,
        in_specs=[smem] * 3 + [vmem] * 6,
        out_specs=[vmem] * 3,
        scratch_shapes=[
            pltpu.VMEM((3 * leaves, 8, size), F32),
            pltpu.VMEM((6, size, size), F32),
            pltpu.VMEM((3, size, size), F32),
            pltpu.VMEM((leaves, 8, size), F32),
            pltpu.VMEM((3 * leaves, 3, 8, size), F32),
        ],
        compiler_params=pltpu.CompilerParams(vmem_limit_bytes=limit),
    )(near_src.T, near_count, first, positions, densities, pos_b, pos_a, dens_b, dens_a)
    return pl.pallas_call(
        functools.partial(far_field, n),
        out_shape=line,
        in_specs=[smem] + [vmem] * 8 + [hbm] * 2,
        out_specs=vmem,
        scratch_shapes=[
            pltpu.VMEM((n, leaves, width), BF16),
            pltpu.VMEM((3, nodes), F32),
            pltpu.VMEM((3, nodes), F32),
            pltpu.VMEM(transfer_table.shape, BF16),
            pltpu.VMEM(down.shape, BF16),
            pltpu.VMEM((far_num * leaves, classes), BF16),
            pltpu.VMEM((cap, far_num * leaves, n), BF16),
            pltpu.VMEM((far_num * leaves, period), F32),
            pltpu.VMEM((leaves, block), F32),
            pltpu.VMEM((block, 128), BF16),
            pltpu.VMEM((leaves, (width + 127) // 128 * 128), F32),
            pltpu.VMEM((3, leaves, size), F32),
            pltpu.SemaphoreType.DMA((blocks,)),
            pltpu.SemaphoreType.DMA,
            pltpu.SemaphoreType.DMA((n,)),
            pltpu.SemaphoreType.DMA((n,)),
            pltpu.SemaphoreType.DMA((2,)),
            pltpu.SemaphoreType.DMA((2,)),
        ],
        compiler_params=pltpu.CompilerParams(
            collective_id=1, has_side_effects=True, vmem_limit_bytes=limit
        ),
    )(
        far_count,
        densities,
        far_slot,
        far_class,
        requests[0].T,
        mom,
        near,
        part_b,
        part_a,
        transfer_table,
        down,
    )


def solution(mesh):
    placed = (
        P(None, "patch"),
        P(None, "patch"),
        P("patch", None),
        P("patch"),
        P("patch", None),
        P("patch", None),
        P("patch"),
        P("patch", None, None),
        P("patch", None, None),
        P(),
        P("patch", None, None, None),
    )
    return jax.shard_map(
        functools.partial(per_device, mesh.shape["patch"]),
        mesh=mesh,
        in_specs=placed,
        out_specs=P(None, "patch"),
        check_vma=False,
    )
```

```python
import functools
import math

import jax
import jax.numpy as jnp
from jax import lax
from jax.experimental import pallas as pl
from jax.experimental.pallas import tpu as pltpu
from jax.sharding import PartitionSpec as P

KERNEL = 1.0 / (8.0 * math.pi)
BLOB = 0.25
MESH = pl.DeviceIdType.MESH
F32 = jnp.float32
BF16 = jnp.bfloat16


def iota(shape, dim):
    return lax.broadcasted_iota(jnp.int32, shape, dim)


def dot(a, b):
    return jnp.dot(a, b, preferred_element_type=F32)


def exchange(
    n,
    pos,
    dens,
    up_hbm,
    pos_b,
    pos_a,
    dens_b,
    dens_a,
    mom,
    up,
    dens_rows,
    local_sem,
    halo_send,
    halo_recv,
):
    leaves, width = mom.shape
    size = pos.shape[1] // leaves
    me = lax.axis_index("patch")
    right = lax.rem(me + 1, n)
    left = lax.rem(me + n - 1, n)
    get_up = pltpu.make_async_copy(up_hbm, up, local_sem)
    get_up.start()
    barrier = pltpu.get_barrier_semaphore()

    for peer in (left, right):
        pl.semaphore_signal(barrier, inc=1, device_id=(peer,), device_id_type=MESH)

    for leaf in range(leaves):
        for c in range(3):
            dens_rows[leaf : leaf + 1, c * size : (c + 1) * size] = dens[
                c : c + 1, leaf * size : (leaf + 1) * size
            ]
    dens_round = dens_rows[...].astype(BF16)
    pl.semaphore_wait(barrier, 2)
    halos = []
    for k, (src, dst, peer) in enumerate(
        ((pos, pos_b, right), (dens, dens_b, right), (pos, pos_a, left), (dens, dens_a, left))
    ):
        copy = pltpu.make_async_remote_copy(
            src_ref=src,
            dst_ref=dst,
            send_sem=halo_send.at[k],
            recv_sem=halo_recv.at[k],
            device_id=(peer,),
            device_id_type=MESH,
        )
        copy.start()
        halos.append(copy)

    get_up.wait()
    row = iota((leaves, width), 0)
    total = jnp.zeros((leaves, width), F32)
    for leaf in range(leaves):
        got = lax.dot_general(
            dens_round, up[leaf], (((1,), (1,)), ((), ())), preferred_element_type=F32
        )
        total = total + jnp.where(row == leaf, got, 0.0)
    mom[...] = total.astype(BF16)

    for copy in halos:
        copy.wait()


def near_field(
    near_src,
    near_count,
    first,
    pos,
    dens,
    pos_b,
    pos_a,
    dens_b,
    dens_a,
    near,
    part_b,
    part_a,
    window,
    tb,
    tacc,
    near_t,
    src_acc,
):
    leaves = near_count.shape[0]
    size = pos.shape[1] // leaves
    src_acc[...] = jnp.zeros_like(src_acc)
    window[...] = jnp.zeros_like(window)
    for part, (x, f) in enumerate(((pos_b, dens_b), (pos, dens), (pos_a, dens_a))):
        for leaf in range(leaves):
            lanes = slice(leaf * size, (leaf + 1) * size)
            window[part * leaves + leaf, 0:3, :] = x[:, lanes]
            window[part * leaves + leaf, 3:6, :] = f[:, lanes]

    offset = first[0]
    lane = iota((size, size), 1)

    @pl.loop(0, leaves)
    def _(leaf):
        columns = jnp.transpose(window[leaves + leaf])
        for c in range(6):
            col = columns[:, c : c + 1]
            if c >= 3:
                col = col * KERNEL
            tb[c] = jnp.broadcast_to(col, (size, size))
        tacc[...] = jnp.zeros_like(tacc)

        def near_block(slot, carry):
            index = near_src[slot, leaf] - offset
            other = window[index]
            xs = [jnp.broadcast_to(other[c : c + 1], (8, size)) for c in range(3)]
            fs = [jnp.broadcast_to(other[c : c + 1], (8, size)) for c in range(3, 6)]
            src_sum = [None] * 3
            for g in range(size // 8):
                r8 = slice(g * 8, (g + 1) * 8)
                ft = [tb[3 + c, r8, :] for c in range(3)]
                sep = [tb[c, r8, :] - xs[c] for c in range(3)]
                rho = sep[0] * sep[0] + sep[1] * sep[1] + sep[2] * sep[2] + BLOB
                inv1 = lax.rsqrt(rho)
                inv2 = inv1 * inv1
                inv3 = inv1 * inv2
                ab = ft[0] * fs[0] + ft[1] * fs[1] + ft[2] * fs[2]
                ar = ft[0] * sep[0] + ft[1] * sep[1] + ft[2] * sep[2]
                br = fs[0] * sep[0] + fs[1] * sep[1] + fs[2] * sep[2]
                p = br * inv3
                q = ar * inv3
                w = ab * inv3 + (3.0 * (p * ar)) * inv2
                for c in range(3):
                    t = ft[c] * p + fs[c] * q - w * sep[c]
                    tacc[c, r8, :] += t
                    src_sum[c] = t if g == 0 else src_sum[c] + t
            for c in range(3):
                src_acc[index, c] += src_sum[c]
            return carry

        lax.fori_loop(0, near_count[leaf], near_block, 0)
        cols = [jnp.sum(tacc[c], axis=1, keepdims=True) for c in range(3)]
        mixed = jnp.where(lane == 0, cols[0], jnp.where(lane == 1, cols[1], cols[2]))
        near_t[leaf] = jnp.transpose(mixed)[0:8]

    for part, buf in ((0, part_b), (2, part_a)):
        for leaf in range(leaves):
            for c in range(3):
                buf[c : c + 1, leaf * size : (leaf + 1) * size] = jnp.sum(
                    src_acc[part * leaves + leaf, c], axis=0, keepdims=True
                )
    for leaf in range(leaves):
        for c in range(3):
            near[c : c + 1, leaf * size : (leaf + 1) * size] = near_t[
                leaf, c : c + 1, :
            ] - jnp.sum(src_acc[leaves + leaf, c], axis=0, keepdims=True)


def far_field(
    n,
    far_count,
    dens,
    far_slot,
    far_class,
    req,
    mom_own,
    near,
    part_b,
    part_a,
    table_hbm,
    down_hbm,
    out,
    mom,
    got_b,
    got_a,
    table,
    down,
    hot_class,
    hot_slot,
    tiled,
    sums,
    fold,
    expan,
    far_acc,
    table_sem,
    down_sem,
    mom_send,
    mom_recv,
    part_send,
    part_recv,
):
    leaves, width = mom_own.shape
    me = lax.axis_index("patch")
    barrier = pltpu.get_barrier_semaphore()

    @pl.loop(1, n)
    def _(k):
        pl.semaphore_signal(
            barrier, inc=1, device_id=(lax.rem(me + k, n),), device_id_type=MESH
        )

    size = dens.shape[1] // leaves
    far_num = far_slot.shape[1]
    classes = table.shape[0]
    cap = req.shape[0]
    block = fold.shape[0]

    def table_copy(b):
        lanes = pl.ds(pl.multiple_of(b * block, 128), block)
        return pltpu.make_async_copy(
            table_hbm.at[:, lanes], table.at[:, lanes], table_sem.at[b]
        )

    for b in range(width * width // block):
        table_copy(b).start()
    get_down = pltpu.make_async_copy(down_hbm, down, down_sem)
    get_down.start()
    count_col = jnp.zeros((leaves, 1), jnp.int32)
    leaf_col = iota((leaves, 1), 0)
    for leaf in range(leaves):
        count_col = jnp.where(leaf_col == leaf, far_count[leaf], count_col)
    class_iota = iota((leaves, classes), 1)
    for s in range(far_num):
        rows = slice(s * leaves, (s + 1) * leaves)
        wanted = jnp.where(s < count_col, far_class[:, s : s + 1], -1)
        hot_class[rows, :] = (class_iota == wanted).astype(F32).astype(BF16)
    fold_row = iota(fold.shape, 0)
    fold_first = iota(fold.shape, 1) * width
    fold[...] = (
        ((fold_row >= fold_first) & (fold_row < fold_first + width)).astype(F32).astype(BF16)
    )
    pl.semaphore_wait(barrier, n - 1)

    def mom_copy(k):
        return pltpu.make_async_remote_copy(
            src_ref=mom_own,
            dst_ref=mom.at[me],
            send_sem=mom_send.at[k],
            recv_sem=mom_recv.at[k],
            device_id=(lax.rem(me + k, n),),
            device_id_type=MESH,
        )

    @pl.loop(1, n)
    def _(k):
        mom_copy(k).start()

    parts = []
    for k, (src, dst, peer) in enumerate(
        (
            (part_b, got_a, lax.rem(me + n - 1, n)),
            (part_a, got_b, lax.rem(me + 1, n)),
        )
    ):
        copy = pltpu.make_async_remote_copy(
            src_ref=src,
            dst_ref=dst,
            send_sem=part_send.at[k],
            recv_sem=part_recv.at[k],
            device_id=(peer,),
            device_id_type=MESH,
        )
        copy.start()
        parts.append(copy)

    mom[me] = mom_own[...]
    column = iota((leaves, cap * n), 1)
    slot_of = lax.rem(column, n) * cap + lax.div(column, n)
    for s in range(far_num):
        rows = slice(s * leaves, (s + 1) * leaves)
        slot = far_slot[:, s : s + 1]
        hot_slot[rows, :] = (slot_of == slot).astype(F32).astype(BF16)
    period = tiled.shape[1]
    spread_gap = iota((width, period), 1) - iota((width, period), 0)
    spread = spread_gap == 0
    for k in range(1, period // width):
        spread = spread | (spread_gap == k * width)
    spread = spread.astype(F32).astype(BF16)

    @pl.loop(1, n)
    def _(k):
        mom_copy(k).wait_recv()

    moments = mom[...].reshape(n * leaves, width)
    leaf_iota = iota((n * leaves, n), 0) - iota((n * leaves, n), 1) * leaves
    picked = []
    for place in range(cap):
        pick = (leaf_iota == req[place : place + 1, :]).astype(F32).astype(BF16)
        chosen = lax.dot_general(
            pick, moments, (((0,), (0,)), ((), ())), preferred_element_type=F32
        ).astype(BF16)
        picked.append(dot(chosen, spread).astype(BF16))
    chosen_rows = jnp.concatenate(picked, axis=0)
    for k in range(period // 128):
        lanes = slice(k * 128, (k + 1) * 128)
        tiled[:, lanes] = dot(hot_slot[...], chosen_rows[:, lanes])

    expan[...] = jnp.zeros_like(expan)
    step = 256 if block % 256 == 0 else 128
    per_block = block // width

    @pl.loop(0, width * width // block)
    def _(b):
        table_copy(b).wait()
        for t in range(block // step):
            start = pl.multiple_of(b * block + t * step, 128)
            oper = dot(hot_class[...], table[:, pl.ds(start, step)])
            for h in range(step // 128):
                at = ((t * step) // 128 + h) % (period // 128)
                acc = None
                for s in range(far_num):
                    rows = slice(s * leaves, (s + 1) * leaves)
                    term = oper[rows, h * 128 : (h + 1) * 128] * tiled[
                        rows, at * 128 : (at + 1) * 128
                    ]
                    acc = term if acc is None else acc + term
                sums[:, t * step + h * 128 : t * step + (h + 1) * 128] = acc
        whole = sums[...]
        high = whole.astype(BF16)
        low = (whole - high.astype(F32)).astype(BF16)
        res = dot(high, fold[...]) + dot(low, fold[...])
        wide = jnp.concatenate([res, jnp.zeros((leaves, expan.shape[1] - 128), F32)], axis=1)
        expan[...] += pltpu.roll(wide, b * per_block, 1)

    expansion = expan[...][:, :width].astype(BF16)
    get_down.wait()
    far_acc[...] = jnp.zeros_like(far_acc)
    leaf_row = iota((leaves, size), 0)

    @pl.loop(0, leaves)
    def _(leaf):
        lanes = pl.ds(pl.multiple_of(leaf * size, size), size)
        own = dens[:, lanes]
        fields = [dot(expansion, down[leaf, q]) for q in range(9)]
        for k in range(3):
            far = (
                own[0:1] * fields[k] + own[1:2] * fields[3 + k] + own[2:3] * fields[6 + k]
            )
            far_acc[k] += jnp.where(leaf_row == leaf, far, 0.0)

    for copy in parts:
        copy.wait_recv()
    for leaf in range(leaves):
        lanes = slice(leaf * size, (leaf + 1) * size)
        for c in range(3):
            came = got_b[c : c + 1, lanes] + got_a[c : c + 1, lanes]
            out[c : c + 1, lanes] = near[c : c + 1, lanes] - came + far_acc[c, leaf : leaf + 1, :]
    for copy in parts:
        copy.wait_send()

    @pl.loop(1, n)
    def _(k):
        mom_copy(k).wait_send()


def per_device(
    n,
    positions,
    densities,
    near_src,
    near_count,
    far_slot,
    far_class,
    far_count,
    requests,
    up_basis,
    transfer_table,
    down_basis,
):
    leaves = near_count.shape[0]
    nodes = positions.shape[1]
    size = nodes // leaves
    width = up_basis.shape[1]
    far_num = far_slot.shape[1]
    cap = requests.shape[2]
    classes = transfer_table.shape[0]
    period = math.lcm(width, 128)
    blocks = width * width // period
    block = 2 * period if blocks % 2 == 0 else period
    down = jnp.transpose(down_basis, (0, 2, 1, 3))
    blocks = width * width // block
    smem = pl.BlockSpec(memory_space=pltpu.SMEM)
    vmem = pl.BlockSpec(memory_space=pltpu.VMEM)
    hbm = pl.BlockSpec(memory_space=pl.ANY)
    line = jax.ShapeDtypeStruct((3, nodes), F32)
    limit = 60 * 1024 * 1024
    pos_b, pos_a, dens_b, dens_a, mom = pl.pallas_call(
        functools.partial(exchange, n),
        out_shape=[line] * 4 + [jax.ShapeDtypeStruct((leaves, width), BF16)],
        in_specs=[vmem] * 2 + [hbm],
        out_specs=[vmem] * 5,
        scratch_shapes=[
            pltpu.VMEM(up_basis.shape, BF16),
            pltpu.VMEM((leaves, 3 * size), F32),
            pltpu.SemaphoreType.DMA,
            pltpu.SemaphoreType.DMA((4,)),
            pltpu.SemaphoreType.DMA((4,)),
        ],
        compiler_params=pltpu.CompilerParams(
            collective_id=0, has_side_effects=True, vmem_limit_bytes=limit
        ),
    )(positions, densities, up_basis)
    first = ((lax.axis_index("patch") - 1) * leaves).reshape(1)
    near, part_b, part_a = pl.pallas_call(
        near_field,
        out_shape=[line] * 3,
        in_specs=[smem] * 3 + [vmem] * 6,
        out_specs=[vmem] * 3,
        scratch_shapes=[
            pltpu.VMEM((3 * leaves, 8, size), F32),
            pltpu.VMEM((6, size, size), F32),
            pltpu.VMEM((3, size, size), F32),
            pltpu.VMEM((leaves, 8, size), F32),
            pltpu.VMEM((3 * leaves, 3, 8, size), F32),
        ],
        compiler_params=pltpu.CompilerParams(vmem_limit_bytes=limit),
    )(near_src.T, near_count, first, positions, densities, pos_b, pos_a, dens_b, dens_a)
    return pl.pallas_call(
        functools.partial(far_field, n),
        out_shape=line,
        in_specs=[smem] + [vmem] * 8 + [hbm] * 2,
        out_specs=vmem,
        scratch_shapes=[
            pltpu.VMEM((n, leaves, width), BF16),
            pltpu.VMEM((3, nodes), F32),
            pltpu.VMEM((3, nodes), F32),
            pltpu.VMEM(transfer_table.shape, BF16),
            pltpu.VMEM(down.shape, BF16),
            pltpu.VMEM((far_num * leaves, classes), BF16),
            pltpu.VMEM((far_num * leaves, cap * n), BF16),
            pltpu.VMEM((far_num * leaves, period), F32),
            pltpu.VMEM((leaves, block), F32),
            pltpu.VMEM((block, 128), BF16),
            pltpu.VMEM((leaves, (width + 127) // 128 * 128), F32),
            pltpu.VMEM((3, leaves, size), F32),
            pltpu.SemaphoreType.DMA((blocks,)),
            pltpu.SemaphoreType.DMA,
            pltpu.SemaphoreType.DMA((n,)),
            pltpu.SemaphoreType.DMA((n,)),
            pltpu.SemaphoreType.DMA((2,)),
            pltpu.SemaphoreType.DMA((2,)),
        ],
        compiler_params=pltpu.CompilerParams(
            collective_id=1, has_side_effects=True, vmem_limit_bytes=limit
        ),
    )(
        far_count,
        densities,
        far_slot,
        far_class,
        requests[0].T,
        mom,
        near,
        part_b,
        part_a,
        transfer_table,
        down,
    )


def solution(mesh):
    placed = (
        P(None, "patch"),
        P(None, "patch"),
        P("patch", None),
        P("patch"),
        P("patch", None),
        P("patch", None),
        P("patch"),
        P("patch", None, None),
        P("patch", None, None),
        P(),
        P("patch", None, None, None),
    )
    return jax.shard_map(
        functools.partial(per_device, mesh.shape["patch"]),
        mesh=mesh,
        in_specs=placed,
        out_specs=P(None, "patch"),
        check_vma=False,
    )
```
